128 devices in a mesh: comp: 2 (over x_lo), tile: 64 (over y, z, x_hi, core).
Axes of the slice: x: 4 (x_hi: 2, x_lo: 2; x = x_hi * 2 + x_lo), y: 4, z: 4, core: 2. Of those that a mesh axis runs over, the one named last changes fastest.
Arguments:
- starting_perturbation: float32 [2, 128, 512, 512], P('comp', None, 'tile'), may hold values from -6 to 6
- measured_discrepancy: float32 [2, 128, 512, 512], P('comp', None, 'tile'), may hold values from -6 to 6
- diffusion: float32 [2, 128, 512, 512], P('comp', None, 'tile'), may hold values from 0.02 to 0.24
- vert_mix: float32 [2, 128, 128], P('comp'), may hold values from -0.03125 to 0.03125
- ocean_mask: int32 [512, 512], P('tile'), may hold values 0 or 1
- pair_tile: int32 [2, 64, 8], replicated, may hold values from 0 to 63, as said below
- pair_patch: int32 [2, 64, 64], replicated, may hold values from 0 to 31
- dest_patch: int32 [2, 64, 64], P('comp', 'tile'), may hold values from 0 to 31
- pair_blocks: int32 [2, 64, 8], P('comp', 'tile'), may hold values from 1 to 8, 48 in all within a row
- remap_weight: float32 [2, 4096, 128, 128], P('comp', 'tile'), may hold values from -0.5 to 0.5
Outputs:
- final_perturbation: float32 [2, 128, 512, 512], P('comp', None, 'tile')
- gradient: float32 [2, 128, 512, 512], P('comp', None, 'tile')
The draws below stay inside these ranges and needn't reach their ends.
Inputs may be any that keep to these rules, and one draw needn't show every extreme that they name: `pair_tile`: the 8 source tiles listed for destination tile t are distinct; exactly one of them is (t + 32) mod 64, and each other is (t + o) mod 64 for some o from 1 - 8 to 7. A pair's live blocks are its first pair_blocks ones.
All inputs are finite; a program needn't handle non-finite values. No bound on the sum of `ocean_mask` on one device may be relied on, other than what follows from the above.
Results may differ from the reference program's by a relative error of at most 0.0001.
Values sent between devices are 32-bit elements; how exact they have to be, the bound alone decides.
A program may use at most 128 MiB of HBM per device.

```python
import math
import jax
import jax.numpy as jnp
import numpy as np
from jax import lax

LEV = 128
LON = 512
STEPS = 4
NPAIR = 8
PB = 8
PATCH = 128
TILES = 64
NROWS = 512
NBLK = 64
NPATCH = 32


def draw_pair_tile(key, part):
    key_list = jax.random.split(jax.random.fold_in(key, 17), 2 * TILES)
    tile_ids = jnp.tile(jnp.arange(TILES, dtype=jnp.int32), 2)

    def draw_row(subkey, tile_now):
        first_key, second_key = jax.random.split(subkey)
        near_offsets = jax.random.permutation(first_key, 2 * NPAIR - 1)[:NPAIR - 1].astype(jnp.int32) - (NPAIR - 1)
        all_offsets = jnp.concatenate([near_offsets, jnp.full((1,), TILES // 2, jnp.int32)])
        ordered = jax.random.permutation(second_key, all_offsets)
        return (tile_now + ordered) % TILES
    return jax.vmap(draw_row)(key_list, tile_ids).reshape(2, TILES, NPAIR).astype(jnp.int32)


def set_ends(values, own_key, smallest, high):
    longest = values.shape.index(max(values.shape))
    spots = []
    for shift in (0, 1):
        where = [jax.random.randint(jax.random.fold_in(own_key, axis), (), 0, length) for axis, length in enumerate(values.shape)]
        where[longest] = (where[longest] + shift) % values.shape[longest]
        spots.append(tuple(where))
    return values.at[spots[0]].set(smallest).at[spots[1]].set(high)


def levels(stream_key, dims, cuts, smallest, top_value):
    level = 1.0
    for axis_at, shards_of in cuts:
        draws = jax.random.uniform(jax.random.fold_in(jax.random.fold_in(stream_key, 6), axis_at), (shards_of,), jnp.float32, smallest / len(cuts), top_value / len(cuts))
        level = level * jnp.repeat(jnp.exp(draws), dims[axis_at] // shards_of).reshape((-1,) + (1,) * (len(dims) - 1 - axis_at))
    return level


def profile(count, total, most, skew):
    weights = [(1 << 20) // math.isqrt(grade ** skew) + 1 for grade in range(2, count + 1)]
    surplus, holding = total - most - (count - 1), [1] * (count - 1)
    while surplus > 0:
        free = [i for i in range(count - 1) if holding[i] < most]
        whole, remaining = sum([weights[i] for i in free]), surplus
        for i in free:
            extra = min(most - holding[i], max(1, remaining * weights[i] // whole), surplus)
            holding[i] = holding[i] + extra
            surplus = surplus - extra
    return np.array([most] + holding)


def ragged(key, count, total, limit, lean):
    if count == 2:
        one = jax.random.randint(key, (), max(1, total - limit), min(limit, total - 1) + 1)
        return jnp.stack([one, total - one])
    lengths = jnp.asarray(profile(count, total, limit, lean), jnp.int32)
    couples = (count - 1) // 2
    giver, sink = lengths[1:1 + 2 * couples:2], lengths[2:2 + 2 * couples:2]
    room = jnp.minimum(giver - 1, limit - sink)
    moved = jax.random.randint(jax.random.fold_in(key, 1), (couples,), 0, 1 << 20) % (room + 1)
    lengths = lengths.at[1:1 + 2 * couples:2].set(giver - moved).at[2:2 + 2 * couples:2].set(sink + moved)
    return lengths[jax.random.permutation(jax.random.fold_in(key, 2), count)]


def gaussian(rng, dims, deviation, limit, cuts=(), kind=jnp.bfloat16):
    level = levels(rng, dims, cuts, -0.22, 0.18) if cuts else 1.0
    drawn = jax.random.normal(rng, dims, jnp.float32) * deviation * level
    return jnp.minimum(jnp.maximum(drawn, -limit), limit).astype(kind)


def setup_inputs(seed: int = 0) -> dict:
    splits = jax.random.split(jax.random.key(seed), 11)
    starting_perturbation = gaussian(splits[0], (2, LEV, NROWS, LON), 1.0, 6.0, ((0, 2), (2, 64)), jnp.float32)
    measured_discrepancy = gaussian(splits[1], (2, LEV, NROWS, LON), 1.0, 6.0, ((0, 2), (2, 64)), jnp.float32)
    diffusion = jnp.clip(jnp.exp(math.log(0.24) - 2.4849066 * jax.random.uniform(splits[2], (2, LEV, NROWS, LON), jnp.float32) ** levels(splits[2], (2, LEV, NROWS, LON), ((0, 2), (2, 64)), -0.2, 0.2)), 0.02, 0.24)
    vert_mix = gaussian(splits[3], (2, LEV, LEV), (256 * LEV) ** -0.5, 0.03125, ((0, 2),), jnp.float32)
    ocean_mask = set_ends((jax.random.randint(splits[4], (NROWS, LON), 0, 10) < 7).astype(jnp.int32), jax.random.fold_in(splits[4], 1), 0, 1)
    pair_tile = draw_pair_tile(jax.random.fold_in(splits[10], 71), 0)
    pair_patch = set_ends(jax.random.randint(splits[6], (2, TILES, NBLK), 0, NPATCH), jax.random.fold_in(splits[6], 1), 0, NPATCH - 1).astype(jnp.int32)
    dest_patch = set_ends(jax.random.randint(splits[7], (2, TILES, NBLK), 0, NPATCH), jax.random.fold_in(splits[7], 1), 0, NPATCH - 1).astype(jnp.int32)
    pair_blocks = jax.vmap(lambda own: ragged(own, NPAIR, NPAIR * PB * 3 // 4, PB, 2))(jax.random.split(splits[8], 2 * TILES)).reshape((2, TILES, NPAIR)).astype(jnp.int32)
    remap_weight = gaussian(splits[9], (2, TILES * NBLK, PATCH, PATCH), PATCH ** -0.5, 0.5, ((0, 2), (1, 64)), jnp.float32)
    return dict(starting_perturbation=starting_perturbation, measured_discrepancy=measured_discrepancy, diffusion=diffusion, vert_mix=vert_mix, ocean_mask=ocean_mask, pair_tile=pair_tile, pair_patch=pair_patch, dest_patch=dest_patch, pair_blocks=pair_blocks, remap_weight=remap_weight)


precise = lax.Precision.HIGHEST

def laplace(system_variables):
    padded = jnp.pad(system_variables, ((0, 0), (0, 0), (1, 1), (0, 0)))
    return padded[:, :, 2:] + padded[:, :, :-2] + jnp.roll(system_variables, -1, axis=3) + jnp.roll(system_variables, 1, axis=3) - 4.0 * system_variables

def column_mix(matrix, system_variables):
    return jnp.einsum('clm,cmrx->clrx', matrix, system_variables, precision=precise)

def reference(starting_perturbation, measured_discrepancy, diffusion, vert_mix, ocean_mask, pair_tile, pair_patch, dest_patch, pair_blocks, remap_weight):
    seawater_indicator = jnp.stack([jnp.ones((NROWS, LON), jnp.float32), ocean_mask.astype(jnp.float32)])[:, None]
    block_ids = jnp.arange(NBLK, dtype=jnp.int32)
    owner_pair = block_ids // PB
    slot_ids = block_ids % PB

    def remap(surface, destination):
        source = surface[1 - destination].reshape(TILES * NPATCH, PATCH)
        source_rows = (pair_tile[destination][:, owner_pair] * NPATCH + pair_patch[destination]).reshape(-1)
        live_mask = (slot_ids[None, :] < pair_blocks[destination][:, owner_pair]).astype(jnp.float32).reshape(-1, 1)
        block_terms = jnp.einsum('bij,bj->bi', remap_weight[destination], source[source_rows], precision=precise) * live_mask
        target = (jnp.arange(TILES, dtype=jnp.int32)[:, None] * NPATCH + dest_patch[destination]).reshape(-1)
        summed_sensitivity = jnp.zeros((TILES * NPATCH, PATCH), jnp.float32).at[target].add(block_terms)
        return summed_sensitivity.reshape(NROWS, LON)

    def couple(system_variables):
        surface = system_variables[:, 0]
        summed_sensitivity = jnp.stack([remap(surface, 0), remap(surface, 1)])
        return system_variables.at[:, 0].add(seawater_indicator[:, 0] * summed_sensitivity)

    def forward_step(system_variables):
        return seawater_indicator * (system_variables + diffusion * laplace(system_variables) + column_mix(vert_mix, system_variables))

    def joint_earth_system(system_variables):
        for step_index in range(STEPS):
            system_variables = forward_step(system_variables)
        system_variables = couple(system_variables)
        for step_index in range(STEPS):
            system_variables = forward_step(system_variables)
        return system_variables
    final_perturbation, reverse_derivative_operator = jax.vjp(joint_earth_system, starting_perturbation)
    measurement_mismatch = final_perturbation - measured_discrepancy
    backpropagated_sensitivity = reverse_derivative_operator(measurement_mismatch)[0]
    return (final_perturbation, starting_perturbation + backpropagated_sensitivity)
```

```python
import jax
import jax.numpy as jnp
from jax import lax
from jax.experimental import pallas as pl
from jax.experimental.pallas import tpu as pltpu
from jax.sharding import PartitionSpec as P

STEPS = 4
LANES = 128
NEAR = 8
FAR = 2 * NEAR - 1

F32 = jnp.float32
BF16 = jnp.bfloat16


def halves(x):
    high = x.astype(BF16)
    return high, (x - high.astype(F32)).astype(BF16)


def mm(a, b):
    return jnp.dot(a, b, preferred_element_type=F32)


def window_kernel(
    tiles,
    start_hbm,
    measured_hbm,
    scaled_hbm,
    weight_hbm,
    sea_ref,
    mix_ref,
    source_col,
    source_row,
    landing_col,
    final_hbm,
    adjoint_hbm,
    v,
    w,
    g,
    scaled,
    measured,
    weights,
    mixed,
    forward_mix,
    forward_low,
    backward_mix,
    backward_low,
    outgoing,
    halo,
    surface,
    arrived,
    parcels,
    returned,
    picked,
    terms,
    load_sem,
    store_sem,
    halo_send,
    halo_recv,
    out_send,
    out_recv,
    back_send,
    back_recv,
):
    rows, levels, lon = scaled.shape
    chunks = lon // LANES
    patches = rows * chunks
    blocks = weights.shape[0]
    slots = 2 * NEAR
    last = rows - 1
    me = lax.axis_index("tile")
    other = 1 - lax.axis_index("comp")
    above = lax.rem(me + tiles - 1, tiles)
    below = lax.rem(me + 1, tiles)
    offsets = [j if j < NEAR else (tiles // 2 if j == FAR else j - FAR) for j in range(slots)]
    keep = (
        jnp.where(me > 0, 1.0, 0.0).astype(F32),
        jnp.where(me < tiles - 1, 1.0, 0.0).astype(F32),
    )

    loads = [
        pltpu.make_async_copy(start_hbm, v.at[0], load_sem.at[0]),
        pltpu.make_async_copy(scaled_hbm, scaled, load_sem.at[1]),
        pltpu.make_async_copy(weight_hbm, weights, load_sem.at[2]),
        pltpu.make_async_copy(measured_hbm, measured, load_sem.at[3]),
    ]
    for load in loads:
        load.start()

    barrier = pltpu.get_barrier_semaphore()
    for neighbour in (above, below):
        pl.semaphore_signal(barrier, inc=1, device_id={"tile": neighbour})
    for offset in offsets:
        pl.semaphore_signal(
            barrier,
            inc=1,
            device_id={"comp": other, "tile": lax.rem(me + offset + tiles, tiles)},
        )

    high, low = halves(mix_ref[...])
    forward_mix[...] = jnp.concatenate([high, high], axis=1)
    forward_low[...] = low
    high, low = halves(mix_ref[...].T)
    backward_mix[...] = jnp.concatenate([high, high], axis=1)
    backward_low[...] = low

    def edge_copy(side, chunk, slot):
        return pltpu.make_async_remote_copy(
            src_ref=outgoing.at[side, chunk],
            dst_ref=halo.at[slot, side, chunk],
            send_sem=halo_send.at[side, chunk],
            recv_sem=halo_recv.at[slot, side, chunk],
            device_id={"tile": below if side == 0 else above},
        )

    def send_edges(field):
        for chunk in range(chunks):
            cols = pl.ds(chunk * LANES, LANES)
            for side, row in ((0, last), (1, 0)):
                outgoing[side, chunk] = field[0, row, :, cols]
                edge_copy(side, chunk, 0).start()

    def column_mix(x, wide, narrow):
        high, low = halves(x)
        mixed[...] = mm(wide[...], jnp.concatenate([high, low], axis=0)) + mm(narrow[...], high)

    def across(x):
        return pltpu.roll(x, 1, 1) + pltpu.roll(x, lon - 1, 1) - 4.0 * x

    depth = 32

    def forward_row(cur, nxt, row, neighbours):
        column_mix(v[cur, row], forward_mix, forward_low)
        sea = sea_ref[pl.ds(row, 1), :]
        for base in range(0, levels, depth):
            band = pl.ds(base, depth)
            x = v[cur, row, band, :]
            total = across(x)
            for step in neighbours:
                total = total + v[cur, row + step, band, :]
            v[nxt, row, band, :] = sea * (x + mixed[band, :]) + scaled[row, band, :] * total

    def backward_row(cur, nxt, row, neighbours):
        sea = sea_ref[pl.ds(row, 1), :]
        column_mix(sea * w[cur, row], backward_mix, backward_low)
        for base in range(0, levels, depth):
            band = pl.ds(base, depth)
            total = across(g[cur, row, band, :])
            for step in neighbours:
                total = total + g[cur, row + step, band, :]
            value = sea * w[cur, row, band, :] + mixed[band, :] + total
            w[nxt, row, band, :] = value
            if len(neighbours) == 2:
                g[nxt, row, band, :] = scaled[row, band, :] * value

    def section(row_update, edge_update):
        def step(k, carry):
            cur = lax.rem(k, 2)
            nxt = 1 - cur
            row_update(cur, nxt, 0, (1,))
            row_update(cur, nxt, last, (-1,))

            def inner(row, carry):
                row_update(cur, nxt, row, (-1, 1))
                return carry

            lax.fori_loop(1, last, inner, 0)
            for chunk in range(chunks):
                cols = pl.ds(chunk * LANES, LANES)
                for arriving, row in ((0, 0), (1, last)):
                    edge_copy(arriving, chunk, cur).wait_recv()
                    leaving = 1 - arriving
                    edge_copy(leaving, chunk, cur).wait_send()
                    outgoing[leaving, chunk] = edge_update(
                        nxt, row, cols, keep[arriving] * halo[cur, arriving, chunk]
                    )

                    @pl.when(k < STEPS - 1)
                    def _():
                        edge_copy(leaving, chunk, nxt).start()

            return carry

        lax.fori_loop(0, STEPS, step, 0)

    def forward_edge(nxt, row, cols, incoming):
        value = v[nxt, row, :, cols] + scaled[row, :, cols] * incoming
        v[nxt, row, :, cols] = value
        return value

    def backward_edge(nxt, row, cols, incoming):
        value = w[nxt, row, :, cols] + incoming
        w[nxt, row, :, cols] = value
        value = scaled[row, :, cols] * value
        g[nxt, row, :, cols] = value
        return value

    places = [
        (row * chunks + chunk, row, pl.ds(chunk * LANES, LANES))
        for row in range(rows)
        for chunk in range(chunks)
    ]

    loads[0].wait()
    pl.semaphore_wait(barrier, slots + 2)
    send_edges(v)
    loads[1].wait()
    section(forward_row, forward_edge)

    for patch, row, cols in places:
        surface[pl.ds(patch, 1), :] = v[0, row, pl.ds(0, 1), cols]
    out_copies = [
        pltpu.make_async_remote_copy(
            src_ref=surface,
            dst_ref=arrived.at[j],
            send_sem=out_send.at[j],
            recv_sem=out_recv.at[j],
            device_id={"comp": other, "tile": lax.rem(me - offset + tiles, tiles)},
        )
        for j, offset in enumerate(offsets)
    ]
    for copy in out_copies:
        copy.start()
    loads[2].wait()
    loads[3].wait()
    landing = (
        lax.broadcasted_iota(jnp.int32, (blocks, LANES), 1) == landing_col[...]
    ).astype(F32)
    for copy in out_copies:
        copy.wait_recv()
    pick = (
        lax.broadcasted_iota(jnp.int32, (blocks, slots * patches), 1) == source_col[...]
    ).astype(F32).astype(BF16)
    high, low = halves(arrived[...].reshape(slots * patches, LANES))
    picked[...] = mm(pick, high) + mm(pick, low)
    terms[...] = landing

    def remap_block(b, total):
        value = weights[b] * picked[pl.ds(b, 1), :]
        return total + jnp.sum(value, axis=1, keepdims=True) * terms[pl.ds(b, 1), :]

    remapped = lax.fori_loop(
        0, blocks, remap_block, jnp.zeros((LANES, LANES), F32), unroll=8
    ).T
    for patch, row, cols in places:
        v[0, row, pl.ds(0, 1), cols] = (
            v[0, row, pl.ds(0, 1), cols]
            + sea_ref[pl.ds(row, 1), cols] * remapped[patch : patch + 1, :]
        )
    for copy in out_copies:
        copy.wait_send()

    send_edges(v)
    section(forward_row, forward_edge)

    store_final = pltpu.make_async_copy(v.at[0], final_hbm, store_sem.at[0])
    store_final.start()

    def mismatch(row, carry):
        value = v[0, row] - measured[row]
        w[0, row] = value
        g[0, row] = scaled[row] * value
        return carry

    lax.fori_loop(0, rows, mismatch, 0)
    send_edges(g)
    section(backward_row, backward_edge)

    for patch, row, cols in places:
        surface[pl.ds(patch, 1), :] = sea_ref[pl.ds(row, 1), cols] * w[0, row, pl.ds(0, 1), cols]
    high, low = halves(surface[...])
    spot = landing[:, :patches].astype(BF16)
    picked[...] = mm(spot, high) + mm(spot, low)

    def return_block(b, carry):
        high, low = halves(picked[pl.ds(b, 1), :])
        weight_high, weight_low = halves(weights[b])
        terms[pl.ds(b, 1), :] = mm(high, weight_high) + mm(low, weight_high) + mm(high, weight_low)
        return carry

    lax.fori_loop(0, blocks, return_block, 0, unroll=8)
    place = (
        lax.broadcasted_iota(jnp.int32, (slots * patches, blocks), 0) == source_row[...]
    ).astype(F32).astype(BF16)
    high, low = halves(terms[...])
    parcels[...] = (mm(place, high) + mm(place, low)).reshape(slots, patches, LANES)
    back_copies = [
        pltpu.make_async_remote_copy(
            src_ref=parcels.at[j],
            dst_ref=returned.at[j],
            send_sem=back_send.at[j],
            recv_sem=back_recv.at[j],
            device_id={"comp": other, "tile": lax.rem(me + offset + tiles, tiles)},
        )
        for j, offset in enumerate(offsets)
    ]
    for copy in back_copies:
        copy.start()
    for copy in back_copies:
        copy.wait_recv()
    surface[...] = jnp.sum(returned[...], axis=0)
    for patch, row, cols in places:
        value = surface[pl.ds(patch, 1), :]
        w[0, row, pl.ds(0, 1), cols] = w[0, row, pl.ds(0, 1), cols] + value
        g[0, row, pl.ds(0, 1), cols] = (
            g[0, row, pl.ds(0, 1), cols] + scaled[row, pl.ds(0, 1), cols] * value
        )
    for copy in back_copies:
        copy.wait_send()

    send_edges(g)
    section(backward_row, backward_edge)
    store_adjoint = pltpu.make_async_copy(w.at[0], adjoint_hbm, store_sem.at[1])
    store_adjoint.start()
    store_final.wait()
    store_adjoint.wait()


def shards(
    starting_perturbation,
    measured_discrepancy,
    diffusion,
    vert_mix,
    ocean_mask,
    pair_tile,
    pair_patch,
    dest_patch,
    pair_blocks,
    remap_weight,
):
    component = lax.axis_index("comp")
    own_tile = lax.axis_index("tile")
    tiles = lax.axis_size("tile")
    levels, rows, lon = starting_perturbation.shape[1:]
    chunks = lon // LANES
    patches = rows * chunks
    blocks = remap_weight.shape[1]
    pairs = pair_tile.shape[2]
    per_pair = blocks // pairs
    slots = 2 * NEAR

    sea = jnp.where(component == 1, ocean_mask.astype(F32), 1.0)
    by_row = lambda x: jnp.transpose(x[0], (1, 0, 2))
    start = by_row(starting_perturbation)
    scaled = by_row(diffusion * sea[None, None])
    measured = by_row(measured_discrepancy)

    offset = (pair_tile[component, own_tile] - own_tile + tiles) % tiles
    slot = jnp.where(
        offset < NEAR, offset, jnp.where(offset == tiles // 2, FAR, offset - tiles + FAR)
    )
    block_ids = jnp.arange(blocks, dtype=jnp.int32)
    live = block_ids % per_pair < jnp.repeat(pair_blocks[0, 0], per_pair)
    source = jnp.repeat(slot, per_pair) * patches + pair_patch[component, own_tile]
    source = jnp.where(live, source, slots * patches)
    landing = dest_patch[0, 0]

    field = (rows, levels, lon)
    hbm = pl.BlockSpec(memory_space=pl.ANY)
    vmem = pl.BlockSpec(memory_space=pltpu.VMEM)
    dma = pltpu.SemaphoreType.DMA
    final, adjoint = pl.pallas_call(
        lambda *refs: window_kernel(tiles, *refs),
        out_shape=(jax.ShapeDtypeStruct(field, F32), jax.ShapeDtypeStruct(field, F32)),
        in_specs=[hbm] * 4 + [vmem] * 5,
        out_specs=(hbm, hbm),
        scratch_shapes=[
            pltpu.VMEM((2,) + field, F32),
            pltpu.VMEM((2,) + field, F32),
            pltpu.VMEM((2,) + field, F32),
            pltpu.VMEM(field, F32),
            pltpu.VMEM(field, F32),
            pltpu.VMEM((blocks, LANES, LANES), F32),
            pltpu.VMEM((levels, lon), F32),
            pltpu.VMEM((levels, 2 * levels), BF16),
            pltpu.VMEM((levels, levels), BF16),
            pltpu.VMEM((levels, 2 * levels), BF16),
            pltpu.VMEM((levels, levels), BF16),
            pltpu.VMEM((2, chunks, levels, LANES), F32),
            pltpu.VMEM((2, 2, chunks, levels, LANES), F32),
            pltpu.VMEM((patches, LANES), F32),
            pltpu.VMEM((slots, patches, LANES), F32),
            pltpu.VMEM((slots, patches, LANES), F32),
            pltpu.VMEM((slots, patches, LANES), F32),
            pltpu.VMEM((blocks, LANES), F32),
            pltpu.VMEM((blocks, LANES), F32),
            dma((4,)),
            dma((2,)),
            dma((2, chunks)),
            dma((2, 2, chunks)),
            dma((slots,)),
            dma((slots,)),
            dma((slots,)),
            dma((slots,)),
        ],
        compiler_params=pltpu.CompilerParams(
            collective_id=0, has_side_effects=True, vmem_limit_bytes=48 * 1024 * 1024
        ),
        name="window",
    )(
        start,
        measured,
        scaled,
        remap_weight[0],
        sea,
        vert_mix[0],
        source[:, None],
        source[None, :],
        landing[:, None],
    )
    back = lambda x: jnp.transpose(x, (1, 0, 2))[None]
    return (back(final), starting_perturbation + back(adjoint))


def solution(mesh):
    placed = (
        P("comp", None, "tile", None),
        P("comp", None, "tile", None),
        P("comp", None, "tile", None),
        P("comp", None, None),
        P("tile", None),
        P(),
        P(),
        P("comp", "tile", None),
        P("comp", "tile", None),
        P("comp", "tile", None, None),
    )
    return jax.shard_map(
        shards,
        mesh=mesh,
        in_specs=placed,
        out_specs=(P("comp", None, "tile", None), P("comp", None, "tile", None)),
        check_vma=False,
    )
```

```python
import jax
import jax.numpy as jnp
from jax import lax
from jax.experimental import pallas as pl
from jax.experimental.pallas import tpu as pltpu
from jax.sharding import PartitionSpec as P

STEPS = 4
LANES = 128
NEAR = 8
FAR = 2 * NEAR - 1
GROUP = 8
PARTS = 2

F32 = jnp.float32
BF16 = jnp.bfloat16


def halves(x):
    high = x.astype(BF16)
    return high, (x - high.astype(F32)).astype(BF16)


def mm(a, b):
    return jnp.dot(a, b, preferred_element_type=F32)


def window_kernel(
    tiles,
    start_hbm,
    measured_hbm,
    diffusion_hbm,
    weight_hbm,
    ocean_hbm,
    mix_hbm,
    pair_tile_hbm,
    pair_patch_hbm,
    dest_patch_hbm,
    pair_blocks_hbm,
    final_hbm,
    gradient_hbm,
    start_raw,
    measured_raw,
    diffusion_raw,
    v,
    w,
    g,
    scaled,
    measured,
    weights,
    sea_ref,
    mixed,
    forward_mix,
    forward_low,
    backward_mix,
    backward_low,
    outgoing,
    halo,
    surface,
    departing,
    arrived,
    parcels,
    returned,
    terms,
    shift_out,
    shift_in,
    picked,
    landing,
    pick,
    place,
    gather,
    collect,
    ocean_ref,
    mix_ref,
    pair_tile,
    pair_patch,
    dest_patch,
    pair_blocks,
    load_sem,
    store_sem,
    halo_send,
    halo_recv,
    out_send,
    out_recv,
    back_send,
    back_recv,
    shift_send,
    shift_recv,
):
    rows, levels, lon = scaled.shape
    chunks = lon // LANES
    blocks = weights.shape[0]
    per_pair = GROUP
    pairs = blocks // per_pair
    slots = 2 * NEAR
    last = rows - 1
    part_levels = levels // PARTS
    me = lax.axis_index("tile")
    component = lax.axis_index("comp")
    other = 1 - component
    above = lax.rem(me + tiles - 1, tiles)
    below = lax.rem(me + 1, tiles)

    offsets = [j if j < NEAR else (tiles // 2 if j == FAR else j - FAR) for j in range(slots)]
    keep = (
        jnp.where(me > 0, 1.0, 0.0).astype(F32),
        jnp.where(me < tiles - 1, 1.0, 0.0).astype(F32),
    )

    loads = [
        pltpu.make_async_copy(start_hbm.at[0], start_raw, load_sem.at[0]),
        pltpu.make_async_copy(diffusion_hbm.at[0], diffusion_raw, load_sem.at[1]),
        pltpu.make_async_copy(measured_hbm.at[0], measured_raw, load_sem.at[2]),
        pltpu.make_async_copy(weight_hbm.at[0], weights, load_sem.at[3]),
        pltpu.make_async_copy(mix_hbm.at[0], mix_ref, load_sem.at[4]),
        pltpu.make_async_copy(ocean_hbm, ocean_ref, load_sem.at[5]),
        pltpu.make_async_copy(pair_tile_hbm, pair_tile, load_sem.at[6]),
        pltpu.make_async_copy(pair_patch_hbm, pair_patch, load_sem.at[7]),
        pltpu.make_async_copy(dest_patch_hbm, dest_patch, load_sem.at[8]),
        pltpu.make_async_copy(pair_blocks_hbm, pair_blocks, load_sem.at[9]),
    ]
    for load in loads:
        load.start()

    barrier = pltpu.get_barrier_semaphore()
    for neighbour in (above, below):
        pl.semaphore_signal(barrier, inc=1, device_id={"tile": neighbour})
    for offset in offsets:
        pl.semaphore_signal(
            barrier,
            inc=1,
            device_id={"comp": other, "tile": lax.rem(me + offset + tiles, tiles)},
        )

    shift_out[...] = jnp.zeros_like(shift_out)
    def edge_copy(side, part, chunk, slot):
        return pltpu.make_async_remote_copy(
            src_ref=outgoing.at[side, part, chunk],
            dst_ref=halo.at[slot, side, part, chunk],
            send_sem=halo_send.at[side, part, chunk],
            recv_sem=halo_recv.at[slot, side, part, chunk],
            device_id={"tile": below if side == 0 else above},
        )

    def send_edges(field, part):
        band = pl.ds(part * part_levels, part_levels)
        for chunk in range(chunks):
            cols = pl.ds(chunk * LANES, LANES)
            for side, row in ((0, last), (1, 0)):
                outgoing[side, part, chunk] = field[0, row, band, cols]
                edge_copy(side, part, chunk, 0).start()

    def shift_copy(phase, side):
        return pltpu.make_async_remote_copy(
            src_ref=shift_out.at[phase, side],
            dst_ref=shift_in.at[phase, side],
            send_sem=shift_send.at[phase, side],
            recv_sem=shift_recv.at[phase, side],
            device_id={"tile": below if side == 0 else above},
        )

    def flip(block):
        return jnp.swapaxes(block, 0, 1)

    def by_level_block(body):
        def step(i, carry):
            body(pl.ds(pl.multiple_of(i * GROUP, GROUP), GROUP))
            return carry

        lax.fori_loop(0, levels // GROUP, step, 0)

    def column_mix(i, x, wide, narrow):
        high, low = halves(x)
        mixed[i] = mm(wide[...], jnp.concatenate([high, low], axis=0)) + mm(narrow[...], high)

    def across(x):
        return pltpu.roll(x, 1, 1) + pltpu.roll(x, lon - 1, 1) - 4.0 * x

    depth = 32

    def forward_rows(cur, nxt, targets):
        for i, (row, _) in enumerate(targets):
            column_mix(i, v[cur, row], forward_mix, forward_low)
        for i, (row, neighbours) in enumerate(targets):
            sea = sea_ref[pl.ds(row, 1), :]
            for base in range(0, levels, depth):
                band = pl.ds(base, depth)
                x = v[cur, row, band, :]
                total = across(x)
                for step in neighbours:
                    total = total + v[cur, row + step, band, :]
                v[nxt, row, band, :] = (
                    sea * (x + mixed[i, band, :]) + scaled[row, band, :] * total
                )

    def backward_rows(cur, nxt, targets):
        for i, (row, _) in enumerate(targets):
            sea = sea_ref[pl.ds(row, 1), :]
            column_mix(i, sea * w[cur, row], backward_mix, backward_low)
        for i, (row, neighbours) in enumerate(targets):
            sea = sea_ref[pl.ds(row, 1), :]
            for base in range(0, levels, depth):
                band = pl.ds(base, depth)
                total = across(g[cur, row, band, :])
                for step in neighbours:
                    total = total + g[cur, row + step, band, :]
                value = sea * w[cur, row, band, :] + mixed[i, band, :] + total
                w[nxt, row, band, :] = value
                if len(neighbours) == 2:
                    g[nxt, row, band, :] = scaled[row, band, :] * value

    def inner_pair(update, cur, nxt, index):
        row = 2 + 2 * index
        update(cur, nxt, ((row, (-1, 1)), (row + 1, (-1, 1))))

    def section(update, edge_update, first, phase, final_edge=None, hook=None, hold=False, go_on=True):
        ending = STEPS - 1

        def pair_loop(lo, hi, src, dst):
            def pair(index, carry):
                inner_pair(update, src, dst, index)
                return carry

            lax.fori_loop(lo, hi, pair, 0)

        if phase is None:
            pair_loop(0, (rows - 4) // 2, 0, 1)

        def step(k, carry):
            cur = lax.rem(k, 2)
            nxt = 1 - cur
            update(
                cur,
                nxt,
                ((0, (1,)), (last, (-1,)), (1, (-1, 1)), (last - 1, (-1, 1))),
            )

            def half(i, carry):
                part = i if first == 0 else PARTS - 1 - i
                band = pl.ds(pl.multiple_of(part * part_levels, part_levels), part_levels)
                turning = jnp.logical_and(k == ending, i == 0)
                if phase is not None:

                    @pl.when(jnp.logical_and(k == 0, part == 0))
                    def _():
                        for side in range(2):
                            shift_copy(phase, side).wait_recv()

                for chunk in range(chunks):
                    cols = pl.ds(chunk * LANES, LANES)
                    for arriving, row in ((0, 0), (1, last)):
                        edge_copy(arriving, part, chunk, cur).wait_recv()
                        leaving = 1 - arriving
                        edge_copy(leaving, part, chunk, cur).wait_send()
                        if phase is not None:

                            @pl.when(jnp.logical_and(k == 0, part == 0))
                            def _():
                                halo[0, arriving, 0, chunk, top, :] = (
                                    halo[0, arriving, 0, chunk, top, :]
                                    + shift_in[phase, arriving, pl.ds(chunk, 1), :]
                                )

                        def emit(edge):
                            outgoing[leaving, part, chunk] = edge(
                                nxt,
                                row,
                                band,
                                cols,
                                keep[arriving] * halo[cur, arriving, part, chunk],
                            )

                        if final_edge is None:
                            emit(edge_update)
                        else:

                            @pl.when(k < ending)
                            def _():
                                emit(edge_update)

                            @pl.when(k == ending)
                            def _():
                                emit(final_edge)

                        if go_on and not hold:
                            edge_copy(leaving, part, chunk, nxt).start()
                        else:

                            @pl.when(jnp.logical_not(turning) if go_on else k < ending)
                            def _():
                                edge_copy(leaving, part, chunk, nxt).start()

                if hook is not None:

                    @pl.when(turning)
                    def _():
                        hook()
                        if hold:
                            for chunk in range(chunks):
                                for side in range(2):
                                    edge_copy(side, part, chunk, nxt).start()

                @pl.when(k < ending)
                def _():
                    if phase is None:
                        inner_pair(update, nxt, cur, i)
                    else:
                        late = jnp.logical_and(k == 0, i == 0)
                        pair_loop(
                            jnp.where(k == 0, 0, i),
                            jnp.where(k == 0, (rows - 4) // 2, i + 1),
                            jnp.where(late, cur, nxt),
                            jnp.where(late, nxt, cur),
                        )

                return carry

            lax.fori_loop(0, PARTS, half, 0)
            return carry

        lax.fori_loop(0, STEPS, step, 0)
        if phase is not None:
            for side in range(2):
                shift_copy(phase, side).wait_send()

    def forward_edge(nxt, row, band, cols, incoming):
        value = v[nxt, row, band, cols] + scaled[row, band, cols] * incoming
        v[nxt, row, band, cols] = value
        return value

    def backward_edge(nxt, row, band, cols, incoming):
        value = w[nxt, row, band, cols] + incoming
        w[nxt, row, band, cols] = value
        value = scaled[row, band, cols] * value
        g[nxt, row, band, cols] = value
        return value

    def turning_edge(nxt, row, band, cols, incoming):
        value = forward_edge(nxt, row, band, cols, incoming) - measured[row, band, cols]
        w[nxt, row, band, cols] = value
        value = scaled[row, band, cols] * value
        g[nxt, row, band, cols] = value
        return value

    places = [
        (row * chunks + chunk, row, chunk, pl.ds(chunk * LANES, LANES))
        for row in range(rows)
        for chunk in range(chunks)
    ]
    top = pl.ds(0, 1)

    loads[0].wait()

    def take_start(band):
        v[0, :, band, :] = flip(start_raw[band])

    by_level_block(take_start)
    pl.semaphore_wait(barrier, slots + 2)
    for part in range(PARTS):
        send_edges(v, part)
    for load in loads[4:]:
        load.wait()
    shift_out[...] = jnp.zeros_like(shift_out)
    sea_ref[...] = jnp.where(component == 1, ocean_ref[...].astype(F32), 1.0)
    high, low = halves(mix_ref[...])
    forward_mix[...] = jnp.concatenate([high, high], axis=1)
    forward_low[...] = low
    high, low = halves(mix_ref[...].T)
    backward_mix[...] = jnp.concatenate([high, high], axis=1)
    backward_low[...] = low
    loads[1].wait()

    def take_diffusion(band):
        block = flip(diffusion_raw[band])
        for row in range(rows):
            scaled[row, band, :] = block[row] * sea_ref[pl.ds(row, 1), :]

    by_level_block(take_diffusion)
    loads[2].wait()

    def take_measured(band):
        measured[:, band, :] = flip(measured_raw[band])

    by_level_block(take_measured)

    def iota(shape, dim):
        return lax.broadcasted_iota(jnp.int32, shape, dim)

    def spread(x, y):
        return lax.dot_general(
            x.astype(F32).astype(BF16),
            y.astype(F32).astype(BF16),
            (((1,), (1,)), ((), ())),
            preferred_element_type=F32,
        )

    exchanged = slots * per_pair
    slot = iota((exchanged, tiles), 0) // per_pair
    shift = jnp.where(
        slot < NEAR, slot, jnp.where(slot == FAR, tiles // 2, slot - FAR)
    )
    asking = lax.rem(me - shift + tiles, tiles)
    asking = jnp.where(iota((exchanged, tiles), 1) == asking, 1, 0)
    hit = spread(asking, jnp.where(pair_tile[other] == me, 1, 0))
    hit = mm(
        hit.astype(BF16),
        jnp.where(iota((pairs, blocks), 1) // per_pair == iota((pairs, blocks), 0), 1.0, 0.0)
        .astype(BF16),
    )
    patch_of = mm(
        asking.astype(F32).astype(BF16), pair_patch[other].astype(F32).astype(BF16)
    )
    same = iota((exchanged, blocks), 0) % per_pair == iota((exchanged, blocks), 1) % per_pair
    patch_of = jnp.sum(
        jnp.where(jnp.logical_and(same, hit > 0.5), patch_of, 0.0), axis=1, keepdims=True
    )
    chosen = jnp.where(
        iota((exchanged, LANES), 1).astype(F32) == patch_of, 1.0, 0.0
    )
    gather[...] = chosen.astype(BF16)
    collect[...] = chosen.T.astype(BF16)

    owner = jnp.where(
        iota((blocks, pairs), 0) // per_pair == iota((blocks, pairs), 1), 1.0, 0.0
    )
    mine = jnp.where(iota((pairs, tiles), 1) == me, pair_tile[component], 0)
    mine = jnp.sum(mine.astype(F32), axis=1, keepdims=True)
    source = mm(
        owner.astype(BF16), jnp.broadcast_to(mine, (pairs, LANES)).astype(BF16)
    ).astype(jnp.int32)
    source = source - me
    source = jnp.where(source < 0, source + tiles, source)
    source = jnp.where(
        source < NEAR, source, jnp.where(source == tiles // 2, FAR, source - tiles + FAR)
    )
    source = source * per_pair + iota((blocks, LANES), 0) % per_pair
    live = jnp.sum(owner * pair_blocks[0].astype(F32), axis=1, keepdims=True)
    live = (iota((blocks, LANES), 0) % per_pair).astype(F32) < live
    chosen = jnp.where(
        jnp.logical_and(live, iota((blocks, LANES), 1) == source), 1.0, 0.0
    )
    pick[...] = chosen.astype(BF16)
    chosen = jnp.concatenate([chosen, jnp.zeros((LANES - blocks, LANES), F32)], axis=0)
    place[...] = chosen.T.astype(BF16)
    spot = jnp.where(
        iota((blocks, blocks), 0) == iota((blocks, blocks), 1), dest_patch[0].astype(F32), 0.0
    )
    spot = jnp.sum(spot, axis=1, keepdims=True)
    landing[...] = jnp.where(iota((blocks, LANES), 1).astype(F32) == spot, 1.0, 0.0)

    def select(chooser, x):
        high, low = halves(x)
        return mm(chooser, high) + mm(chooser, low)

    def slot_rows(j):
        return pl.ds(j * per_pair, per_pair)

    def slot_copies(src, dst, send_sem, recv_sem, sign):
        return [
            pltpu.make_async_remote_copy(
                src_ref=src.at[slot_rows(j)],
                dst_ref=dst.at[slot_rows(j)],
                send_sem=send_sem.at[j],
                recv_sem=recv_sem.at[j],
                device_id={"comp": other, "tile": lax.rem(me + sign * offset + tiles, tiles)},
            )
            for j, offset in enumerate(offsets)
        ]

    def give_surface():
        for patch, row, _, cols in places:
            surface[pl.ds(patch, 1), :] = v[0, row, top, cols]

        departing[...] = select(gather[:, : rows * chunks], surface[...])
        for copy in slot_copies(departing, arrived, out_send, out_recv, -1):
            copy.start()

    section(forward_rows, forward_edge, 0, None, hook=give_surface, hold=True)
    loads[3].wait()
    for copy in slot_copies(departing, arrived, out_send, out_recv, -1):
        copy.wait()
    picked[...] = select(pick[...], arrived[...])

    def remap_block(b, total):
        value = weights[b] * picked[pl.ds(b, 1), :]
        return total + jnp.sum(value, axis=1, keepdims=True) * landing[pl.ds(b, 1), :]

    remapped = lax.fori_loop(
        0, blocks, remap_block, jnp.zeros((LANES, LANES), F32), unroll=8
    ).T

    def shift_edges(phase, value, row, chunk):
        for side, edge in ((0, last), (1, 0)):
            if row == edge:
                shift_out[phase, side, pl.ds(chunk, 1), :] = value

    for patch, row, chunk, cols in places:
        value = sea_ref[pl.ds(row, 1), cols] * remapped[patch : patch + 1, :]
        v[0, row, top, cols] = v[0, row, top, cols] + value
        shift_edges(0, value, row, chunk)
    for side in range(2):
        shift_copy(0, side).start()

    section(forward_rows, forward_edge, 1, 0, final_edge=turning_edge)

    def mismatch(row, carry):
        value = v[0, row] - measured[row]
        w[0, row] = value
        g[0, row] = scaled[row] * value
        return carry

    lax.fori_loop(1, last, mismatch, 0)

    def give_final(band):
        diffusion_raw[band] = flip(v[0, :, band, :])

    by_level_block(give_final)
    stores = [pltpu.make_async_copy(diffusion_raw, final_hbm.at[0], store_sem.at[0])]
    stores[0].start()

    def return_block(b, carry):
        high, low = halves(picked[pl.ds(b, 1), :])
        weight_high, weight_low = halves(weights[b])
        terms[pl.ds(b, 1), :] = (
            mm(high, weight_high) + mm(low, weight_high) + mm(high, weight_low)
        )
        return carry

    def give_terms():
        for patch, row, _, cols in places:
            surface[pl.ds(patch, 1), :] = (
                sea_ref[pl.ds(row, 1), cols] * w[0, row, top, cols]
            )
        picked[...] = select(landing[:, : rows * chunks].astype(BF16), surface[...])
        lax.fori_loop(0, blocks, return_block, 0, unroll=8)
        parcels[...] = select(place[:, :blocks], terms[...])
        for copy in slot_copies(parcels, returned, back_send, back_recv, 1):
            copy.start()

    section(backward_rows, backward_edge, 0, None, hook=give_terms)
    for copy in slot_copies(parcels, returned, back_send, back_recv, 1):
        copy.wait()
    surface[...] = select(collect[: rows * chunks, :], returned[...])
    for patch, row, chunk, cols in places:
        value = surface[pl.ds(patch, 1), :]
        w[0, row, top, cols] = w[0, row, top, cols] + value
        value = scaled[row, top, cols] * value
        g[0, row, top, cols] = g[0, row, top, cols] + value
        shift_edges(1, value, row, chunk)
    for side in range(2):
        shift_copy(1, side).start()

    section(backward_rows, backward_edge, 1, 1, go_on=False)

    cuts = 4
    for cut in range(cuts):
        depth_cut = levels // cuts

        def give_gradient(i, carry):
            band = pl.ds(pl.multiple_of(cut * depth_cut + i * GROUP, GROUP), GROUP)
            measured_raw[band] = start_raw[band] + flip(w[0, :, band, :])
            return carry

        lax.fori_loop(0, depth_cut // GROUP, give_gradient, 0)
        part = pl.ds(cut * depth_cut, depth_cut)
        store = pltpu.make_async_copy(
            measured_raw.at[part], gradient_hbm.at[0, part], store_sem.at[1 + cut]
        )
        store.start()
        stores.append(store)
    for store in stores:
        store.wait()


def shards(
    starting_perturbation,
    measured_discrepancy,
    diffusion,
    vert_mix,
    ocean_mask,
    pair_tile,
    pair_patch,
    dest_patch,
    pair_blocks,
    remap_weight,
):
    tiles = lax.axis_size("tile")
    levels, rows, lon = starting_perturbation.shape[1:]
    chunks = lon // LANES
    patches = rows * chunks
    blocks = remap_weight.shape[1]
    slots = 2 * NEAR
    exchanged = slots * GROUP
    part_levels = levels // PARTS

    raw = (levels, rows, lon)
    field = (rows, levels, lon)
    hbm = pl.BlockSpec(memory_space=pltpu.HBM)
    dma = pltpu.SemaphoreType.DMA
    out = jax.ShapeDtypeStruct((1,) + raw, F32)
    return pl.pallas_call(
        lambda *refs: window_kernel(tiles, *refs),
        out_shape=(out, out),
        in_specs=[hbm] * 10,
        out_specs=(hbm, hbm),
        scratch_shapes=[
            pltpu.VMEM(raw, F32),
            pltpu.VMEM(raw, F32),
            pltpu.VMEM(raw, F32),
            pltpu.VMEM((2,) + field, F32),
            pltpu.VMEM((2,) + field, F32),
            pltpu.VMEM((2,) + field, F32),
            pltpu.VMEM(field, F32),
            pltpu.VMEM(field, F32),
            pltpu.VMEM((blocks, LANES, LANES), F32),
            pltpu.VMEM((rows, lon), F32),
            pltpu.VMEM((4, levels, lon), F32),
            pltpu.VMEM((levels, 2 * levels), BF16),
            pltpu.VMEM((levels, levels), BF16),
            pltpu.VMEM((levels, 2 * levels), BF16),
            pltpu.VMEM((levels, levels), BF16),
            pltpu.VMEM((2, PARTS, chunks, part_levels, LANES), F32),
            pltpu.VMEM((2, 2, PARTS, chunks, part_levels, LANES), F32),
            pltpu.VMEM((patches, LANES), F32),
            pltpu.VMEM((exchanged, LANES), F32),
            pltpu.VMEM((exchanged, LANES), F32),
            pltpu.VMEM((exchanged, LANES), F32),
            pltpu.VMEM((exchanged, LANES), F32),
            pltpu.VMEM((blocks, LANES), F32),
            pltpu.VMEM((2, 2, 8, LANES), F32),
            pltpu.VMEM((2, 2, 8, LANES), F32),
            pltpu.VMEM((blocks, LANES), F32),
            pltpu.VMEM((blocks, LANES), F32),
            pltpu.VMEM((blocks, LANES), BF16),
            pltpu.VMEM((LANES, LANES), BF16),
            pltpu.VMEM((LANES, LANES), BF16),
            pltpu.VMEM((LANES, LANES), BF16),
            pltpu.VMEM((rows, lon), jnp.int32),
            pltpu.VMEM((levels, levels), F32),
            pltpu.VMEM((2, pair_tile.shape[2], tiles), jnp.int32),
            pltpu.VMEM(pair_patch.shape, jnp.int32),
            pltpu.VMEM(dest_patch.shape, jnp.int32),
            pltpu.VMEM(pair_blocks.shape, jnp.int32),
            dma((10,)),
            dma((5,)),
            dma((2, PARTS, chunks)),
            dma((2, 2, PARTS, chunks)),
            dma((slots,)),
            dma((slots,)),
            dma((slots,)),
            dma((slots,)),
            dma((2, 2)),
            dma((2, 2)),
        ],
        compiler_params=pltpu.CompilerParams(
            collective_id=0, has_side_effects=True, vmem_limit_bytes=59 * 1024 * 1024
        ),
        name="window",
    )(
        starting_perturbation,
        measured_discrepancy,
        diffusion,
        remap_weight,
        ocean_mask,
        vert_mix,
        jnp.swapaxes(pair_tile, 1, 2),
        pair_patch,
        dest_patch,
        pair_blocks,
    )


def solution(mesh):
    placed = (
        P("comp", None, "tile", None),
        P("comp", None, "tile", None),
        P("comp", None, "tile", None),
        P("comp", None, None),
        P("tile", None),
        P(),
        P(),
        P("comp", "tile", None),
        P("comp", "tile", None),
        P("comp", "tile", None, None),
    )
    return jax.shard_map(
        shards,
        mesh=mesh,
        in_specs=placed,
        out_specs=(P("comp", None, "tile", None), P("comp", None, "tile", None)),
        check_vma=False,
    )
```

```python
import jax
import jax.numpy as jnp
from jax import lax
from jax.experimental import pallas as pl
from jax.experimental.pallas import tpu as pltpu
from jax.sharding import PartitionSpec as P

STEPS = 4
LANES = 128
NEAR = 8
FAR = 2 * NEAR - 1
GROUP = 8
PARTS = 2

F32 = jnp.float32
BF16 = jnp.bfloat16


def halves(x):
    high = x.astype(BF16)
    return high, (x - high.astype(F32)).astype(BF16)


def mm(a, b):
    return jnp.dot(a, b, preferred_element_type=F32)


def window_kernel(
    tiles,
    start_hbm,
    measured_hbm,
    diffusion_hbm,
    weight_hbm,
    ocean_hbm,
    mix_hbm,
    pair_tile_hbm,
    pair_patch_hbm,
    dest_patch_hbm,
    pair_blocks_hbm,
    final_hbm,
    gradient_hbm,
    start_raw,
    measured_raw,
    diffusion_raw,
    v,
    w,
    g,
    scaled,
    measured,
    weights,
    sea_ref,
    mixed,
    forward_mix,
    forward_low,
    backward_mix,
    backward_low,
    outgoing,
    halo,
    surface,
    departing,
    arrived,
    parcels,
    returned,
    terms,
    shift_out,
    shift_in,
    picked,
    landing,
    pick,
    place,
    gather,
    collect,
    ocean_ref,
    mix_ref,
    pair_tile,
    pair_patch,
    dest_patch,
    pair_blocks,
    load_sem,
    store_sem,
    halo_send,
    halo_recv,
    out_send,
    out_recv,
    back_send,
    back_recv,
    shift_send,
    shift_recv,
):
    rows, levels, lon = scaled.shape
    chunks = lon // LANES
    blocks = weights.shape[0]
    per_pair = GROUP
    pairs = blocks // per_pair
    slots = 2 * NEAR
    last = rows - 1
    part_levels = levels // PARTS
    me = lax.axis_index("tile")
    component = lax.axis_index("comp")
    other = 1 - component
    above = lax.rem(me + tiles - 1, tiles)
    below = lax.rem(me + 1, tiles)

    offsets = [j if j < NEAR else (tiles // 2 if j == FAR else j - FAR) for j in range(slots)]
    keep = (
        jnp.where(me > 0, 1.0, 0.0).astype(F32),
        jnp.where(me < tiles - 1, 1.0, 0.0).astype(F32),
    )

    loads = [
        pltpu.make_async_copy(
            start_hbm.at[0, pl.ds(0, part_levels)],
            start_raw.at[pl.ds(0, part_levels)],
            load_sem.at[0],
        ),
        pltpu.make_async_copy(diffusion_hbm.at[0], diffusion_raw, load_sem.at[1]),
        pltpu.make_async_copy(measured_hbm.at[0], measured_raw, load_sem.at[2]),
        pltpu.make_async_copy(weight_hbm.at[0], weights, load_sem.at[3]),
        pltpu.make_async_copy(mix_hbm.at[0], mix_ref, load_sem.at[4]),
        pltpu.make_async_copy(ocean_hbm, ocean_ref, load_sem.at[5]),
        pltpu.make_async_copy(pair_tile_hbm, pair_tile, load_sem.at[6]),
        pltpu.make_async_copy(pair_patch_hbm, pair_patch, load_sem.at[7]),
        pltpu.make_async_copy(dest_patch_hbm, dest_patch, load_sem.at[8]),
        pltpu.make_async_copy(pair_blocks_hbm, pair_blocks, load_sem.at[9]),
    ]
    rest = pl.ds(part_levels, levels - part_levels)
    load_rest = pltpu.make_async_copy(
        start_hbm.at[0, rest], start_raw.at[rest], load_sem.at[10]
    )
    loads[0].start()
    load_rest.start()
    for load in loads[1:]:
        load.start()

    barrier = pltpu.get_barrier_semaphore()
    for neighbour in (above, below):
        pl.semaphore_signal(barrier, inc=1, device_id={"tile": neighbour})
    for offset in offsets:
        pl.semaphore_signal(
            barrier,
            inc=1,
            device_id={"comp": other, "tile": lax.rem(me + offset + tiles, tiles)},
        )

    shift_out[...] = jnp.zeros_like(shift_out)
    def edge_copy(side, part, chunk, slot):
        return pltpu.make_async_remote_copy(
            src_ref=outgoing.at[side, part, chunk],
            dst_ref=halo.at[slot, side, part, chunk],
            send_sem=halo_send.at[side, part, chunk],
            recv_sem=halo_recv.at[slot, side, part, chunk],
            device_id={"tile": below if side == 0 else above},
        )

    def send_edges(field, part):
        band = pl.ds(part * part_levels, part_levels)
        for chunk in range(chunks):
            cols = pl.ds(chunk * LANES, LANES)
            for side, row in ((0, last), (1, 0)):
                outgoing[side, part, chunk] = field[0, row, band, cols]
                edge_copy(side, part, chunk, 0).start()

    def shift_copy(phase, side):
        return pltpu.make_async_remote_copy(
            src_ref=shift_out.at[phase, side],
            dst_ref=shift_in.at[phase, side],
            send_sem=shift_send.at[phase, side],
            recv_sem=shift_recv.at[phase, side],
            device_id={"tile": below if side == 0 else above},
        )

    def flip(block):
        return jnp.swapaxes(block, 0, 1)

    def by_level_block(body, lo=0, hi=None):
        def step(i, carry):
            body(pl.ds(pl.multiple_of(i * GROUP, GROUP), GROUP))
            return carry

        lax.fori_loop(lo // GROUP, (levels if hi is None else hi) // GROUP, step, 0)

    def column_mix(i, x, wide, narrow):
        high, low = halves(x)
        mixed[i] = mm(wide[...], jnp.concatenate([high, low], axis=0)) + mm(narrow[...], high)

    def across(x):
        return pltpu.roll(x, 1, 1) + pltpu.roll(x, lon - 1, 1) - 4.0 * x

    depth = 32

    def forward_rows(cur, nxt, targets):
        for i, (row, _) in enumerate(targets):
            column_mix(i, v[cur, row], forward_mix, forward_low)
        for i, (row, neighbours) in enumerate(targets):
            sea = sea_ref[pl.ds(row, 1), :]
            for base in range(0, levels, depth):
                band = pl.ds(base, depth)
                x = v[cur, row, band, :]
                total = across(x)
                for step in neighbours:
                    total = total + v[cur, row + step, band, :]
                v[nxt, row, band, :] = (
                    sea * (x + mixed[i, band, :]) + scaled[row, band, :] * total
                )

    def backward_rows(cur, nxt, targets):
        for i, (row, _) in enumerate(targets):
            sea = sea_ref[pl.ds(row, 1), :]
            column_mix(i, sea * w[cur, row], backward_mix, backward_low)
        for i, (row, neighbours) in enumerate(targets):
            sea = sea_ref[pl.ds(row, 1), :]
            for base in range(0, levels, depth):
                band = pl.ds(base, depth)
                total = across(g[cur, row, band, :])
                for step in neighbours:
                    total = total + g[cur, row + step, band, :]
                value = sea * w[cur, row, band, :] + mixed[i, band, :] + total
                w[nxt, row, band, :] = value
                if len(neighbours) == 2:
                    g[nxt, row, band, :] = scaled[row, band, :] * value

    def inner_pair(update, cur, nxt, index):
        row = 2 + 2 * index
        update(cur, nxt, ((row, (-1, 1)), (row + 1, (-1, 1))))

    def section(update, edge_update, first, phase, final_edge=None, hook=None, hold=False, go_on=True, idle=()):
        ending = STEPS - 1

        def step(k, carry):
            cur = lax.rem(k, 2)
            nxt = 1 - cur
            update(
                cur,
                nxt,
                ((0, (1,)), (last, (-1,))),
            )

            def half(i, carry):
                part = i if first == 0 else PARTS - 1 - i
                band = pl.ds(pl.multiple_of(part * part_levels, part_levels), part_levels)
                turning = jnp.logical_and(k == ending, i == 0)
                if phase is not None:

                    @pl.when(jnp.logical_and(k == 0, part == 0))
                    def _():
                        for side in range(2):
                            shift_copy(phase, side).wait_recv()

                for chunk in range(chunks):
                    cols = pl.ds(chunk * LANES, LANES)
                    for arriving, row in ((0, 0), (1, last)):
                        edge_copy(arriving, part, chunk, cur).wait_recv()
                        leaving = 1 - arriving
                        edge_copy(leaving, part, chunk, cur).wait_send()
                        if phase is not None:

                            @pl.when(jnp.logical_and(k == 0, part == 0))
                            def _():
                                halo[0, arriving, 0, chunk, top, :] = (
                                    halo[0, arriving, 0, chunk, top, :]
                                    + shift_in[phase, arriving, pl.ds(chunk, 1), :]
                                )

                        def emit(edge):
                            outgoing[leaving, part, chunk] = edge(
                                nxt,
                                row,
                                band,
                                cols,
                                keep[arriving] * halo[cur, arriving, part, chunk],
                            )

                        if final_edge is None:
                            emit(edge_update)
                        else:

                            @pl.when(k < ending)
                            def _():
                                emit(edge_update)

                            @pl.when(k == ending)
                            def _():
                                emit(final_edge)

                        if go_on and not hold:
                            edge_copy(leaving, part, chunk, nxt).start()
                        else:

                            @pl.when(jnp.logical_not(turning) if go_on else k < ending)
                            def _():
                                edge_copy(leaving, part, chunk, nxt).start()

                    if chunk == 0:

                        @pl.when(i == 0)
                        def _():
                            update(cur, nxt, ((1, (-1, 1)), (last - 1, (-1, 1))))

                        for when, work in enumerate(idle):

                            @pl.when(jnp.logical_and(k == when + 1, i == PARTS - 1))
                            def _():
                                work()

                    elif chunk <= (rows - 4) // 2:
                        early = jnp.logical_or(k == 0, i == 0)

                        @pl.when(jnp.logical_and(k < ending, early))
                        def _():
                            late = jnp.logical_and(k == 0, i == 0)
                            inner_pair(
                                update,
                                jnp.where(late, cur, nxt),
                                jnp.where(late, nxt, cur),
                                chunk - 1,
                            )

                if hook is not None:

                    @pl.when(turning)
                    def _():
                        hook()
                        if hold:
                            for chunk in range(chunks):
                                for side in range(2):
                                    edge_copy(side, part, chunk, nxt).start()

                return carry

            lax.fori_loop(0, PARTS, half, 0)
            return carry

        lax.fori_loop(0, STEPS, step, 0)
        if phase is not None:
            for side in range(2):
                shift_copy(phase, side).wait_send()

    def forward_edge(nxt, row, band, cols, incoming):
        value = v[nxt, row, band, cols] + scaled[row, band, cols] * incoming
        v[nxt, row, band, cols] = value
        return value

    def backward_edge(nxt, row, band, cols, incoming):
        value = w[nxt, row, band, cols] + incoming
        w[nxt, row, band, cols] = value
        value = scaled[row, band, cols] * value
        g[nxt, row, band, cols] = value
        return value

    def turning_edge(nxt, row, band, cols, incoming):
        value = forward_edge(nxt, row, band, cols, incoming) - measured[row, band, cols]
        w[nxt, row, band, cols] = value
        value = scaled[row, band, cols] * value
        g[nxt, row, band, cols] = value
        return value

    places = [
        (row * chunks + chunk, row, chunk, pl.ds(chunk * LANES, LANES))
        for row in range(rows)
        for chunk in range(chunks)
    ]
    top = pl.ds(0, 1)

    loads[0].wait()

    def take_start(band):
        v[0, :, band, :] = flip(start_raw[band])

    by_level_block(take_start, 0, part_levels)
    pl.semaphore_wait(barrier, slots + 2)
    send_edges(v, 0)
    load_rest.wait()
    by_level_block(take_start, part_levels)
    for part in range(1, PARTS):
        send_edges(v, part)
    for load in loads[4:]:
        load.wait()
    shift_out[...] = jnp.zeros_like(shift_out)
    sea_ref[...] = jnp.where(component == 1, ocean_ref[...].astype(F32), 1.0)
    high, low = halves(mix_ref[...])
    forward_mix[...] = jnp.concatenate([high, high], axis=1)
    forward_low[...] = low
    high, low = halves(mix_ref[...].T)
    backward_mix[...] = jnp.concatenate([high, high], axis=1)
    backward_low[...] = low
    loads[1].wait()

    def take_diffusion(band):
        block = flip(diffusion_raw[band])
        for row in range(rows):
            scaled[row, band, :] = block[row] * sea_ref[pl.ds(row, 1), :]

    by_level_block(take_diffusion)

    def take_measured(band):
        measured[:, band, :] = flip(measured_raw[band])

    def measured_rows():
        loads[2].wait()
        by_level_block(take_measured)

    def iota(shape, dim):
        return lax.broadcasted_iota(jnp.int32, shape, dim)

    def spread(x, y):
        return lax.dot_general(
            x.astype(F32).astype(BF16),
            y.astype(F32).astype(BF16),
            (((1,), (1,)), ((), ())),
            preferred_element_type=F32,
        )

    def selections():
        exchanged = slots * per_pair
        slot = iota((exchanged, tiles), 0) // per_pair
        shift = jnp.where(
            slot < NEAR, slot, jnp.where(slot == FAR, tiles // 2, slot - FAR)
        )
        asking = lax.rem(me - shift + tiles, tiles)
        asking = jnp.where(iota((exchanged, tiles), 1) == asking, 1, 0)
        hit = spread(asking, jnp.where(pair_tile[other] == me, 1, 0))
        hit = mm(
            hit.astype(BF16),
            jnp.where(iota((pairs, blocks), 1) // per_pair == iota((pairs, blocks), 0), 1.0, 0.0)
            .astype(BF16),
        )
        patch_of = mm(
            asking.astype(F32).astype(BF16), pair_patch[other].astype(F32).astype(BF16)
        )
        same = iota((exchanged, blocks), 0) % per_pair == iota((exchanged, blocks), 1) % per_pair
        patch_of = jnp.sum(
            jnp.where(jnp.logical_and(same, hit > 0.5), patch_of, 0.0), axis=1, keepdims=True
        )
        chosen = jnp.where(
            iota((exchanged, LANES), 1).astype(F32) == patch_of, 1.0, 0.0
        )
        gather[...] = chosen.astype(BF16)
        collect[...] = chosen.T.astype(BF16)

        owner = jnp.where(
            iota((blocks, pairs), 0) // per_pair == iota((blocks, pairs), 1), 1.0, 0.0
        )
        mine = jnp.where(iota((pairs, tiles), 1) == me, pair_tile[component], 0)
        mine = jnp.sum(mine.astype(F32), axis=1, keepdims=True)
        source = mm(
            owner.astype(BF16), jnp.broadcast_to(mine, (pairs, LANES)).astype(BF16)
        ).astype(jnp.int32)
        source = source - me
        source = jnp.where(source < 0, source + tiles, source)
        source = jnp.where(
            source < NEAR, source, jnp.where(source == tiles // 2, FAR, source - tiles + FAR)
        )
        source = source * per_pair + iota((blocks, LANES), 0) % per_pair
        live = jnp.sum(owner * pair_blocks[0].astype(F32), axis=1, keepdims=True)
        live = (iota((blocks, LANES), 0) % per_pair).astype(F32) < live
        chosen = jnp.where(
            jnp.logical_and(live, iota((blocks, LANES), 1) == source), 1.0, 0.0
        )
        pick[...] = chosen.astype(BF16)
        chosen = jnp.concatenate([chosen, jnp.zeros((LANES - blocks, LANES), F32)], axis=0)
        place[...] = chosen.T.astype(BF16)
        spot = jnp.where(
            iota((blocks, blocks), 0) == iota((blocks, blocks), 1), dest_patch[0].astype(F32), 0.0
        )
        spot = jnp.sum(spot, axis=1, keepdims=True)
        landing[...] = jnp.where(iota((blocks, LANES), 1).astype(F32) == spot, 1.0, 0.0)

    def select(chooser, x):
        high, low = halves(x)
        return mm(chooser, high) + mm(chooser, low)

    def slot_rows(j):
        return pl.ds(j * per_pair, per_pair)

    def slot_copies(src, dst, send_sem, recv_sem, sign):
        return [
            pltpu.make_async_remote_copy(
                src_ref=src.at[slot_rows(j)],
                dst_ref=dst.at[slot_rows(j)],
                send_sem=send_sem.at[j],
                recv_sem=recv_sem.at[j],
                device_id={"comp": other, "tile": lax.rem(me + sign * offset + tiles, tiles)},
            )
            for j, offset in enumerate(offsets)
        ]

    def give_surface():
        for patch, row, _, cols in places:
            surface[pl.ds(patch, 1), :] = v[0, row, top, cols]

        departing[...] = select(gather[:, : rows * chunks], surface[...])
        for copy in slot_copies(departing, arrived, out_send, out_recv, -1):
            copy.start()

    section(
        forward_rows,
        forward_edge,
        0,
        None,
        hook=give_surface,
        hold=True,
        idle=(measured_rows, selections),
    )
    loads[3].wait()
    for copy in slot_copies(departing, arrived, out_send, out_recv, -1):
        copy.wait()
    picked[...] = select(pick[...], arrived[...])

    def remap_block(b, total):
        value = weights[b] * picked[pl.ds(b, 1), :]
        return total + jnp.sum(value, axis=1, keepdims=True) * landing[pl.ds(b, 1), :]

    remapped = lax.fori_loop(
        0, blocks, remap_block, jnp.zeros((LANES, LANES), F32), unroll=16
    ).T

    def shift_edges(phase, value, row, chunk):
        for side, edge in ((0, last), (1, 0)):
            if row == edge:
                shift_out[phase, side, pl.ds(chunk, 1), :] = value

    for patch, row, chunk, cols in places:
        value = sea_ref[pl.ds(row, 1), cols] * remapped[patch : patch + 1, :]
        v[0, row, top, cols] = v[0, row, top, cols] + value
        shift_edges(0, value, row, chunk)
    for side in range(2):
        shift_copy(0, side).start()

    section(forward_rows, forward_edge, 1, 0, final_edge=turning_edge)

    def mismatch(row, carry):
        value = v[0, row] - measured[row]
        w[0, row] = value
        g[0, row] = scaled[row] * value
        return carry

    lax.fori_loop(1, last, mismatch, 0)

    def give_final(band):
        diffusion_raw[band] = flip(v[0, :, band, :])

    stores = [pltpu.make_async_copy(diffusion_raw, final_hbm.at[0], store_sem.at[0])]

    def final_rows():
        by_level_block(give_final)
        stores[0].start()


    def return_block(b, carry):
        high, low = halves(picked[pl.ds(b, 1), :])
        weight_high, weight_low = halves(weights[b])
        terms[pl.ds(b, 1), :] = (
            mm(high, weight_high) + mm(low, weight_high) + mm(high, weight_low)
        )
        return carry

    def give_terms():
        for patch, row, _, cols in places:
            surface[pl.ds(patch, 1), :] = (
                sea_ref[pl.ds(row, 1), cols] * w[0, row, top, cols]
            )
        picked[...] = select(landing[:, : rows * chunks].astype(BF16), surface[...])
        lax.fori_loop(0, blocks, return_block, 0, unroll=16)
        parcels[...] = select(place[:, :blocks], terms[...])
        for copy in slot_copies(parcels, returned, back_send, back_recv, 1):
            copy.start()

    section(
        backward_rows, backward_edge, 0, None, hook=give_terms, idle=(final_rows,)
    )
    for copy in slot_copies(parcels, returned, back_send, back_recv, 1):
        copy.wait()
    surface[...] = select(collect[: rows * chunks, :], returned[...])
    for patch, row, chunk, cols in places:
        value = surface[pl.ds(patch, 1), :]
        w[0, row, top, cols] = w[0, row, top, cols] + value
        value = scaled[row, top, cols] * value
        g[0, row, top, cols] = g[0, row, top, cols] + value
        shift_edges(1, value, row, chunk)
    for side in range(2):
        shift_copy(1, side).start()

    section(backward_rows, backward_edge, 1, 1, go_on=False)

    cuts = 4
    for cut in range(cuts):
        depth_cut = levels // cuts

        def give_gradient(i, carry):
            band = pl.ds(pl.multiple_of(cut * depth_cut + i * GROUP, GROUP), GROUP)
            measured_raw[band] = start_raw[band] + flip(w[0, :, band, :])
            return carry

        lax.fori_loop(0, depth_cut // GROUP, give_gradient, 0)
        part = pl.ds(cut * depth_cut, depth_cut)
        store = pltpu.make_async_copy(
            measured_raw.at[part], gradient_hbm.at[0, part], store_sem.at[1 + cut]
        )
        store.start()
        stores.append(store)
    for store in stores:
        store.wait()


def shards(
    starting_perturbation,
    measured_discrepancy,
    diffusion,
    vert_mix,
    ocean_mask,
    pair_tile,
    pair_patch,
    dest_patch,
    pair_blocks,
    remap_weight,
):
    tiles = lax.axis_size("tile")
    levels, rows, lon = starting_perturbation.shape[1:]
    chunks = lon // LANES
    patches = rows * chunks
    blocks = remap_weight.shape[1]
    slots = 2 * NEAR
    exchanged = slots * GROUP
    part_levels = levels // PARTS

    raw = (levels, rows, lon)
    field = (rows, levels, lon)
    hbm = pl.BlockSpec(memory_space=pltpu.HBM)
    dma = pltpu.SemaphoreType.DMA
    out = jax.ShapeDtypeStruct((1,) + raw, F32)
    return pl.pallas_call(
        lambda *refs: window_kernel(tiles, *refs),
        out_shape=(out, out),
        in_specs=[hbm] * 10,
        out_specs=(hbm, hbm),
        scratch_shapes=[
            pltpu.VMEM(raw, F32),
            pltpu.VMEM(raw, F32),
            pltpu.VMEM(raw, F32),
            pltpu.VMEM((2,) + field, F32),
            pltpu.VMEM((2,) + field, F32),
            pltpu.VMEM((2,) + field, F32),
            pltpu.VMEM(field, F32),
            pltpu.VMEM(field, F32),
            pltpu.VMEM((blocks, LANES, LANES), F32),
            pltpu.VMEM((rows, lon), F32),
            pltpu.VMEM((4, levels, lon), F32),
            pltpu.VMEM((levels, 2 * levels), BF16),
            pltpu.VMEM((levels, levels), BF16),
            pltpu.VMEM((levels, 2 * levels), BF16),
            pltpu.VMEM((levels, levels), BF16),
            pltpu.VMEM((2, PARTS, chunks, part_levels, LANES), F32),
            pltpu.VMEM((2, 2, PARTS, chunks, part_levels, LANES), F32),
            pltpu.VMEM((patches, LANES), F32),
            pltpu.VMEM((exchanged, LANES), F32),
            pltpu.VMEM((exchanged, LANES), F32),
            pltpu.VMEM((exchanged, LANES), F32),
            pltpu.VMEM((exchanged, LANES), F32),
            pltpu.VMEM((blocks, LANES), F32),
            pltpu.VMEM((2, 2, 8, LANES), F32),
            pltpu.VMEM((2, 2, 8, LANES), F32),
            pltpu.VMEM((blocks, LANES), F32),
            pltpu.VMEM((blocks, LANES), F32),
            pltpu.VMEM((blocks, LANES), BF16),
            pltpu.VMEM((LANES, LANES), BF16),
            pltpu.VMEM((LANES, LANES), BF16),
            pltpu.VMEM((LANES, LANES), BF16),
            pltpu.VMEM((rows, lon), jnp.int32),
            pltpu.VMEM((levels, levels), F32),
            pltpu.VMEM((2, pair_tile.shape[2], tiles), jnp.int32),
            pltpu.VMEM(pair_patch.shape, jnp.int32),
            pltpu.VMEM(dest_patch.shape, jnp.int32),
            pltpu.VMEM(pair_blocks.shape, jnp.int32),
            dma((11,)),
            dma((5,)),
            dma((2, PARTS, chunks)),
            dma((2, 2, PARTS, chunks)),
            dma((slots,)),
            dma((slots,)),
            dma((slots,)),
            dma((slots,)),
            dma((2, 2)),
            dma((2, 2)),
        ],
        compiler_params=pltpu.CompilerParams(
            collective_id=0, has_side_effects=True, vmem_limit_bytes=59 * 1024 * 1024
        ),
        name="window",
    )(
        starting_perturbation,
        measured_discrepancy,
        diffusion,
        remap_weight,
        ocean_mask,
        vert_mix,
        jnp.swapaxes(pair_tile, 1, 2),
        pair_patch,
        dest_patch,
        pair_blocks,
    )


def solution(mesh):
    placed = (
        P("comp", None, "tile", None),
        P("comp", None, "tile", None),
        P("comp", None, "tile", None),
        P("comp", None, None),
        P("tile", None),
        P(),
        P(),
        P("comp", "tile", None),
        P("comp", "tile", None),
        P("comp", "tile", None, None),
    )
    return jax.shard_map(
        shards,
        mesh=mesh,
        in_specs=placed,
        out_specs=(P("comp", None, "tile", None), P("comp", None, "tile", None)),
        check_vma=False,
    )
```
